32 devices in a mesh: gx: 4 (over z), gy: 4 (over y, core), gz: 2 (over x).
Axes of the slice: x: 2, y: 2, z: 4, core: 2. Of those that a mesh axis runs over, the one named last changes fastest.
Arguments:
- volume: bfloat16 [32, 64, 32, 128], P('gx', 'gy', 'gz'), may hold values from -6 to 6
- w_full: bfloat16 [3, 3, 3, 128, 128], replicated, may hold values from -0.15625 to 0.15625
- w_half: bfloat16 [3, 3, 3, 128, 256], replicated, may hold values from -0.15625 to 0.15625
- w_bottom_in: bfloat16 [3, 3, 3, 256, 512], P(None, None, None, None, 'gx'), may hold values from -0.109375 to 0.109375
- w_bottom_out: bfloat16 [3, 3, 3, 512, 512], P(None, None, None, None, 'gx'), may hold values from -0.078125 to 0.078125
- w_up: bfloat16 [3, 3, 3, 768, 256], replicated, may hold values from -0.0625 to 0.0625
Outputs:
- decoded: bfloat16 [16, 32, 16, 256], P('gx', 'gy', 'gz')
The draws below stay inside these ranges and needn't reach their ends.
All inputs are finite; a program needn't handle non-finite values.
Results may differ from the reference program's by a relative error of at most 0.009.
Values may be sent and summed in bfloat16 or wider, within the bound.
A program may use at most 64 MiB of HBM per device.

```python
import jax
import jax.numpy as jnp
from jax import lax

C0 = 128
C1 = 256
C2 = 512
NX = 32
NY = 64
NZ = 32


def block_levels(own_key, shape, cuts, least, top_value):
    def one(dim, blocks):
        draws = jax.random.uniform(jax.random.fold_in(jax.random.fold_in(own_key, 6), dim), (blocks,), jnp.float32, least / len(cuts), top_value / len(cuts))
        return jnp.repeat(jnp.exp(draws), shape[dim] // blocks).reshape((-1,) + (1,) * (len(shape) - dim - 1))

    gain = one(*cuts[0])
    for cut in cuts[1:]:
        gain = gain * one(*cut)
    return gain


def normal_values(own_key, dims, scale, reach, cuts=(), held_as=jnp.bfloat16):
    array = scale * jax.random.normal(own_key, dims, jnp.float32)
    if cuts:
        array = array * block_levels(own_key, dims, cuts, -0.22, 0.18)
    return jnp.clip(array, -reach, reach).astype(held_as)


def setup_inputs(seed: int = 0) -> dict:
    keys = jax.random.split(jax.random.key(seed), 7)
    return {
        "volume": normal_values(keys[0], (NX, NY, NZ, C0), 1.0, 6.0, ((0, 4), (1, 4), (2, 2))),
        "w_full": normal_values(keys[1], (3, 3, 3, C0, C0), (27 * C0 // 2) ** -0.5, 0.15625),
        "w_half": normal_values(keys[2], (3, 3, 3, C0, C1), (27 * C0 // 2) ** -0.5, 0.15625),
        "w_bottom_in": normal_values(keys[3], (3, 3, 3, C1, C2), (27 * C1 // 2) ** -0.5, 0.109375, ((4, 4),)),
        "w_bottom_out": normal_values(keys[4], (3, 3, 3, C2, C2), (27 * C2 // 2) ** -0.5, 0.078125, ((4, 4),)),
        "w_up": normal_values(keys[5], (3, 3, 3, C2 + C1, C1), (27 * (C2 + C1) // 2) ** -0.5, 0.0625),
    }


def convolve(field, kernel):
    result = lax.conv_general_dilated(field[None], kernel, (1, 1, 1), "SAME", dimension_numbers=("NDHWC", "DHWIO", "NDHWC"), preferred_element_type=jnp.float32)
    return result[0]


def rectify(total):
    return jnp.maximum(total, 0.0).astype(jnp.bfloat16)


def shrink(field):
    size_x, size_y, size_z, channels = field.shape
    blocks = field.reshape(size_x // 2, 2, size_y // 2, 2, size_z // 2, 2, channels)
    return jnp.max(blocks, axis=(1, 3, 5))


def enlarge(field):
    size_x, size_y, size_z, channels = field.shape
    spread = jnp.broadcast_to(field[:, None, :, None, :, None, :], (size_x, 2, size_y, 2, size_z, 2, channels))
    return spread.reshape(2 * size_x, 2 * size_y, 2 * size_z, channels)


def reference(volume, w_full, w_half, w_bottom_in, w_bottom_out, w_up):
    full_level = rectify(convolve(volume, w_full))
    pooled = shrink(full_level)
    skip_level = rectify(convolve(pooled, w_half))
    coarse = shrink(skip_level)
    bottom_first = rectify(convolve(coarse, w_bottom_in))
    bottom_second = rectify(convolve(bottom_first, w_bottom_out))
    joined = jnp.concatenate([enlarge(bottom_second), skip_level], axis=3)
    return convolve(joined, w_up).astype(jnp.bfloat16)
```

```python
import functools

import jax
import jax.numpy as jnp
from jax import lax
from jax.experimental import pallas as pl
from jax.experimental.pallas import tpu as pltpu
from jax.sharding import PartitionSpec as P

F32 = jnp.float32
BF16 = jnp.bfloat16
STEPS = [(dx, dy) for dx in (-1, 0, 1) for dy in (-1, 0, 1)]


def span(d, n, pad):
    if d == 0:
        return pl.ds(pad, n), pl.ds(1, n)
    if d < 0:
        return pl.ds(pad, 1), pl.ds(n + 1, 1)
    return pl.ds(pad + n - 1, 1), pl.ds(0, 1)


def kernel(
    dims,
    v, wf_h, wh_h, w1_h, w2_h, wu_h,
    out,
    wf, wh, w1, w2, wu, wsem,
    p1, f1, g1, e1, t1,
    p2, f2, g2, e2,
    p3, f3, g3, e3, acc,
    pk2, l2, sel2, q2, pk3, l3, q3, pk4, l4, vup,
    s1, r1, s2, r2, s3, r3, s4, r4, s5, r5, s6, r6,
):
    gxn, gyn = dims
    gx, gy, gz = lax.axis_index("gx"), lax.axis_index("gy"), lax.axis_index("gz")
    oz = 1 - gz

    loads = [
        pltpu.make_async_copy(src, dst, wsem.at[i])
        for i, (src, dst) in enumerate(((wf_h, wf), (wh_h, wh), (w1_h, w1), (w2_h, w2), (wu_h, wu)))
    ]
    for load in loads:
        load.start()

    def on(cond, fn):
        if cond is True:
            fn()
        else:
            pl.when(cond)(fn)

    def exists(dx, dy):
        conds = []
        if dx < 0:
            conds.append(gx > 0)
        if dx > 0:
            conds.append(gx < gxn - 1)
        if dy < 0:
            conds.append(gy > 0)
        if dy > 0:
            conds.append(gy < gyn - 1)
        if not conds:
            return True
        return functools.reduce(jnp.logical_and, conds)

    for ref in (p1, g1, p2, g2, p3, g3, l2, l3, l4):
        ref[...] = jnp.zeros(ref.shape, ref.dtype)

    barrier = pltpu.get_barrier_semaphore()
    for s in range(gxn):
        there = lax.rem(gx + s, gxn)
        for dy in (-1, 0, 1):
            for z in (0, 1):
                if s == 0 and dy == 0 and z == 0:
                    continue

                def signal(there=there, dy=dy, z=z):
                    pl.semaphore_signal(
                        barrier, inc=1,
                        device_id={"gx": there, "gy": gy + dy, "gz": oz if z else gz},
                        device_id_type=pl.DeviceIdType.MESH,
                    )

                on(exists(0, dy), signal)
    lines = 1 + (gy > 0).astype(jnp.int32) + (gy < gyn - 1).astype(jnp.int32)
    pl.semaphore_wait(barrier, 2 * gxn * lines - 1)

    def send(src, dst, ss, rs, x, y, z):
        return pltpu.make_async_remote_copy(
            src_ref=src, dst_ref=dst, send_sem=ss, recv_sem=rs,
            device_id={"gx": x, "gy": y, "gz": z}, device_id_type=pl.DeviceIdType.MESH,
        )

    late = []

    def neighbours(src, pad, face, rim, side, nx, ny, ss, rs):
        arrivals = []
        for i, (dx, dy) in enumerate(STEPS):
            sx, tx = span(dx, nx, pad)
            sy, ty = span(dy, ny, pad)
            fx, _ = span(dx, nx, 0)
            fy, _ = span(dy, ny, 0)
            copies = [send(face.at[fx, fy], side.at[tx, ty], ss.at[9 + i], rs.at[9 + i], gx + dx, gy + dy, oz)]
            if (dx, dy) != (0, 0):
                copies.append(send(src.at[sx, sy], rim.at[tx, ty], ss.at[i], rs.at[i], gx + dx, gy + dy, gz))
            for copy in copies:
                on(exists(dx, dy), copy.start)
                late.append((exists(dx, dy), copy.wait_send))
                arrivals.append((exists(-dx, -dy), copy.wait_recv))

        def wait():
            for cond, fn in arrivals:
                on(cond, fn)

        return wait

    def edge(block):
        size = block.shape[-2]
        rows = lax.broadcasted_iota(jnp.int32, block.shape, block.ndim - 2)
        return jnp.sum(jnp.where(rows == (size - 1) * oz, block, 0.0), axis=block.ndim - 2, keepdims=True)

    def shifted(block, fill):
        size = block.shape[-2]
        axis = block.ndim - 2
        rows = lax.broadcasted_iota(jnp.int32, block.shape, axis)
        below = jnp.where(rows == 0, 0.0, pltpu.roll(block, 1, axis))
        above = jnp.where(rows == size - 1, 0.0, pltpu.roll(block, size - 1, axis))
        if fill is not None:
            fill = jnp.broadcast_to(fill, block.shape)
            below = jnp.where(rows == jnp.where(gz == 1, 0, -1), fill, below)
            above = jnp.where(rows == jnp.where(gz == 0, size - 1, -1), fill, above)
        return below, above

    def rounded(x):
        return x.astype(BF16).astype(F32)

    nx, ny, nz, c0 = v.shape
    for x in range(nx):
        f1[x] = edge(v[x].astype(F32))
    arrived = neighbours(v, 0, f1, p1, g1, nx, ny, s1, r1)
    p1[1 : nx + 1, 1 : ny + 1] = v[...]
    arrived()

    @pl.loop(0, nx + 2)
    def _(x):
        block = p1[x].astype(F32)
        below, above = shifted(block, g1[x])
        e1[x, :, :, 0:c0] = below.astype(BF16)
        e1[x, :, :, c0 : 2 * c0] = p1[x]
        e1[x, :, :, 2 * c0 :] = above.astype(BF16)

    loads[0].wait()

    def full_row(x):
        total = jnp.zeros((ny * nz, c0), F32)
        for ox in range(3):
            for oy in range(3):
                lhs = e1[x + ox, oy : oy + ny].reshape(ny * nz, 3 * c0)
                total = total + jnp.dot(lhs, wf[ox * 3 + oy], preferred_element_type=F32)
        return jnp.maximum(total, 0.0)

    hx, hy, hz = nx // 2, ny // 2, nz // 2

    @pl.loop(0, hx)
    def _(x):
        both = jnp.maximum(full_row(2 * x), full_row(2 * x + 1)).reshape(hy, 2, nz, c0)
        t1[...] = jnp.max(both, axis=1)
        small = jnp.maximum(t1[:, pl.ds(0, hz, stride=2), :], t1[:, pl.ds(1, hz, stride=2), :])
        small = rounded(small)
        p2[x + 1, 1 : hy + 1] = small
        f2[x] = edge(small)

    arrived = neighbours(p2, 1, f2, p2, g2, hx, hy, s2, r2)
    arrived()
    for x in range(hx + 2):
        block = p2[x]
        below, above = shifted(block, g2[x])
        e2[0, x], e2[1, x], e2[2, x] = below, block, above
    loads[1].wait()
    rows = hx * hy * hz
    c1 = wh.shape[2]
    total = jnp.zeros((rows, c1), F32)
    for ox in range(3):
        for oy in range(3):
            for k in range(3):
                lhs = e2[k, ox : ox + hx, oy : oy + hy].reshape(rows, c0).astype(BF16)
                total = total + jnp.dot(lhs, wh[(ox * 3 + oy) * 3 + k], preferred_element_type=F32)
    skip = rounded(jnp.maximum(total, 0.0)).reshape(hx, hy, hz, c1)
    p3[1 : hx + 1, 1 : hy + 1] = skip
    f3[...] = edge(skip)

    cx, cy, cz = hx // 2, hy // 2, hz // 2
    ax = gxn * cx
    group = cz * cx
    m = jnp.max(skip.reshape(cx, 2, cy, 2, hz, c1), axis=(1, 3))
    m = m.reshape(cx * cy * hz, c1)
    m = jnp.maximum(m, pltpu.roll(m, m.shape[0] - 1, 0)).astype(BF16)

    blocks = []
    lane = lax.broadcasted_iota(jnp.int32, (group, cx * cy * hz), 1)
    sub = lax.broadcasted_iota(jnp.int32, (group, cx * cy * hz), 0)
    shift_x = cx.bit_length() - 1
    sub_x = sub & (cx - 1)
    sub_o = sub >> shift_x
    for y in range(cy):
        blocks.append(jnp.where(lane == (sub_x * cy + y) * hz + 2 * sub_o, 1.0, 0.0))
    blocks.append(jnp.where(lane == (sub_x * cy + sub_o) * hz + 2 * (cz - 1) * oz, 1.0, 0.0))
    pick = jnp.concatenate(blocks, axis=0).astype(BF16)
    packets = jnp.dot(pick, m, preferred_element_type=F32).reshape(cy + 1, group, c1).astype(BF16)
    pk2[...] = packets
    l2[gx, 0:cy] = packets[0:cy]

    slots = cy + 5

    def coarse_copy(s, dy, z, k):
        def make(src_gx, tgt_gx):
            if z == 0:
                src = {0: pl.ds(0, cy), -1: pl.ds(0, 1), 1: pl.ds(cy - 1, 1)}[dy]
                dst = {0: pl.ds(0, cy), 1: pl.ds(cy, 1), -1: pl.ds(cy + 1, 1)}[dy]
            else:
                src = pl.ds(cy, 1)
                dst = {0: pl.ds(cy + 2, 1), 1: pl.ds(cy + 3, 1), -1: pl.ds(cy + 4, 1)}[dy]
            return send(pk2.at[src], l2.at[src_gx, dst], s4.at[s, k], r4.at[s, k], tgt_gx, gy + dy, oz if z else gz)

        return make

    def deep_copy(pk, land, ss, rs):
        def choose(s, dy, z, k):
            def make(src_gx, tgt_gx):
                sy, ty = span(dy, cy, 0)
                sender = gz if src_gx is gx else (oz if z else gz)
                if z == 0:
                    src = pk.at[sy]
                    dst = land.at[src_gx, ty, pl.ds(1, cz)]
                else:
                    src = pk.at[sy, pl.ds((cz - 1) * (1 - sender), 1)]
                    dst = land.at[src_gx, ty, pl.ds((cz + 1) * sender, 1)]
                return send(src, dst, ss.at[s, k], rs.at[s, k], tgt_gx, gy + dy, oz if z else gz)

            return make

        return choose

    def column_exchange(choose):
        arrivals = []
        for s in list(range(1, gxn)) + [0]:
            there = lax.rem(gx + s, gxn)
            origin = lax.rem(gx + gxn - s, gxn)
            for k, (dy, z) in enumerate(((0, 0), (-1, 0), (1, 0), (0, 1), (-1, 1), (1, 1))):
                if s == 0 and k == 0:
                    continue
                make = choose(s, dy, z, k)
                copy = make(gx, there)
                on(exists(0, dy), copy.start)
                late.append((exists(0, dy), copy.wait_send))
                arrivals.append((exists(0, -dy), make(origin, there).wait_recv))

        def wait():
            for cond, fn in arrivals:
                on(cond, fn)

        return wait

    arrived = column_exchange(coarse_copy)
    skip_arrived = neighbours(p3, 1, f3, p3, g3, hx, hy, s3, r3)

    span_g = slots * group
    width = gxn * span_g
    lane = lax.broadcasted_iota(jnp.int32, (ax, width), 1)
    xs = lax.broadcasted_iota(jnp.int32, (ax, width), 0)
    base = lane - ((xs >> shift_x) * span_g + (xs & (cx - 1)))
    for y in range(-1, cy + 1):
        for z in range(-1, cz + 1):
            if 0 <= z < cz:
                slot = y if 0 <= y < cy else (cy if y < 0 else cy + 1)
                at = slot * group + z * cx
            else:
                slot = cy + 2 if 0 <= y < cy else (cy + 3 if y < 0 else cy + 4)
                line = y if 0 <= y < cy else (cy - 1 if y < 0 else 0)
                mine = (gz == 1) if z < 0 else (gz == 0)
                at = jnp.where(mine, slot * group + line * cx, -width * 4)
            sel2[y + 1, z + 1] = jnp.where(base == at, 1.0, 0.0)

    rim = (cy + 2) * (cz + 2) * ax
    select = sel2[...].reshape(rim, width).astype(BF16)
    arrived()
    landed = l2[...].astype(F32).reshape(width, c1).astype(BF16)
    block = jnp.dot(select, landed, preferred_element_type=F32).reshape(cy + 2, cz + 2, ax, c1)

    def spread(q, block):
        below, above = shifted(block, None)
        q[0], q[1], q[2] = below, block, above

    deep = cy * cz * ax
    fo = w1.shape[2]

    def bottom(q, w):
        total = jnp.zeros((deep, fo), F32)
        for ox in range(3):
            for oy in range(3):
                for k in range(3):
                    lhs = q[ox, oy : oy + cy, k : k + cz].reshape(deep, q.shape[-1]).astype(BF16)
                    total = total + jnp.dot(lhs, w[(ox * 3 + oy) * 3 + k], preferred_element_type=F32)
        return jnp.maximum(total, 0.0).reshape(cy, cz, ax, fo).astype(BF16)

    spread(q2, block)
    loads[2].wait()
    first = bottom(q2, w1)
    pk3[...] = first
    l3[gx, 1 : cy + 1, 1 : cz + 1] = first
    arrived = column_exchange(deep_copy(pk3, l3, s5, r5))

    skip_arrived()
    for x in range(hx + 2):
        block = p3[x]
        below, above = shifted(block, g3[x])
        e3[0, x], e3[1, x], e3[2, x] = below, block, above
    loads[4].wait()
    c2 = w2.shape[1]
    total = jnp.zeros((rows, c1), F32)
    for ox in range(3):
        for oy in range(3):
            for k in range(3):
                lhs = e3[k, ox : ox + hx, oy : oy + hy].reshape(rows, c1).astype(BF16)
                total = total + jnp.dot(lhs, wu[(ox * 3 + oy) * 3 + k, c2:, :], preferred_element_type=F32)
    acc[...] = total.reshape(hx, hy, hz, c1)

    arrived()
    spread(q3, jnp.concatenate([l3[g].astype(F32) for g in range(gxn)], axis=-1))
    loads[3].wait()
    second = bottom(q3, w2)
    pk4[...] = second
    l4[gx, 1 : cy + 1, 1 : cz + 1] = second
    arrived = column_exchange(deep_copy(pk4, l4, s6, r6))

    lane = lax.broadcasted_iota(jnp.int32, (hz, (cz + 2) * ax), 1)
    zs = lax.broadcasted_iota(jnp.int32, (hz, (cz + 2) * ax), 0)
    blocks = []
    for k in range(3):
        for x in range(-1, hx + 1):
            at = gx * cx + (x >> 1)
            at = jnp.where(jnp.logical_and(at >= 0, at < ax), at, -(cz + 3) * ax)
            blocks.append(jnp.where(lane == ((zs + (k + 1)) >> 1) * ax + at, 1.0, 0.0))
    pick = jnp.concatenate(blocks, axis=0).astype(BF16)

    arrived()
    for y in range(cy + 2):
        field = jnp.concatenate([l4[g, y].astype(F32) for g in range(gxn)], axis=-1)
        field = field.reshape((cz + 2) * ax, c2).astype(BF16)
        vup[:, y] = jnp.dot(pick, field, preferred_element_type=F32).reshape(3, hx + 2, hz, c2)

    parts = []
    for oy in range(3):
        low, high = (oy + 1) // 2, (hy - 1 + oy + 1) // 2 + 1
        count = high - low
        total = jnp.zeros((count * hx * hz, c1), F32)
        for ox in range(3):
            for k in range(3):
                lhs = vup[k, low:high, ox : ox + hx].reshape(count * hx * hz, c2).astype(BF16)
                total = total + jnp.dot(lhs, wu[(ox * 3 + oy) * 3 + k, :c2, :], preferred_element_type=F32)
        parts.append((low, total.reshape(count, hx, hz, c1)))
    for y in range(hy):
        line = acc[:, y]
        for oy in range(3):
            low, part = parts[oy]
            line = line + part[(y + oy + 1) // 2 - low]
        out[:, y] = line.astype(BF16)

    for cond, fn in late:
        on(cond, fn)


def on_device(dims, volume, w_full, w_half, w_bottom_in, w_bottom_out, w_up):
    gxn, gyn = dims
    nx, ny, nz, c0 = volume.shape
    c1 = w_half.shape[4]
    c2, fo = w_bottom_out.shape[3:]
    hx, hy, hz = nx // 2, ny // 2, nz // 2
    cx, cy, cz = hx // 2, hy // 2, hz // 2
    ax = gxn * cx
    weights = [
        w_full.reshape(9, 3 * c0, c0),
        w_half.reshape(27, c0, c1),
        w_bottom_in.reshape(27, c1, fo),
        w_bottom_out.reshape(27, c2, fo),
        w_up.reshape(27, c2 + c1, c1),
    ]
    vm = pltpu.VMEM
    dma = pltpu.SemaphoreType.DMA
    scratch = [vm(w.shape, BF16) for w in weights] + [dma((5,))]
    scratch += [
        vm((nx + 2, ny + 2, nz, c0), BF16), vm((nx, ny, 1, c0), F32), vm((nx + 2, ny + 2, 1, c0), F32),
        vm((nx + 2, ny + 2, nz, 3 * c0), BF16), vm((hy, nz, c0), F32),
        vm((hx + 2, hy + 2, hz, c0), F32), vm((hx, hy, 1, c0), F32), vm((hx + 2, hy + 2, 1, c0), F32),
        vm((3, hx + 2, hy + 2, hz, c0), F32),
        vm((hx + 2, hy + 2, hz, c1), F32), vm((hx, hy, 1, c1), F32), vm((hx + 2, hy + 2, 1, c1), F32),
        vm((3, hx + 2, hy + 2, hz, c1), F32), vm((hx, hy, hz, c1), F32),
        vm((cy + 1, cz * cx, c1), BF16), vm((gxn, cy + 5, cz * cx, c1), BF16),
        vm((cy + 2, cz + 2, ax, gxn * (cy + 5) * cz * cx), F32), vm((3, cy + 2, cz + 2, ax, c1), F32),
        vm((cy, cz, ax, fo), BF16), vm((gxn, cy + 2, cz + 2, ax, fo), BF16), vm((3, cy + 2, cz + 2, ax, c2), F32),
        vm((cy, cz, ax, fo), BF16), vm((gxn, cy + 2, cz + 2, ax, fo), BF16),
        vm((3, cy + 2, hx + 2, hz, c2), F32),
    ]
    scratch += [dma((18,))] * 6 + [dma((gxn, 6))] * 6
    return pl.pallas_call(
        functools.partial(kernel, dims),
        out_shape=jax.ShapeDtypeStruct((hx, hy, hz, c1), BF16),
        in_specs=[pl.BlockSpec(memory_space=pltpu.VMEM)] + [pl.BlockSpec(memory_space=pl.ANY)] * 5,
        out_specs=pl.BlockSpec(memory_space=pltpu.VMEM),
        scratch_shapes=scratch,
        compiler_params=pltpu.CompilerParams(
            collective_id=0, has_side_effects=True, vmem_limit_bytes=60 * 1024 * 1024
        ),
    )(volume, *weights)


def solution(mesh):
    dims = (mesh.shape["gx"], mesh.shape["gy"])
    assert mesh.shape["gz"] == 2
    return jax.shard_map(
        functools.partial(on_device, dims),
        mesh=mesh,
        in_specs=(
            P("gx", "gy", "gz", None),
            P(),
            P(),
            P(None, None, None, None, "gx"),
            P(None, None, None, None, "gx"),
            P(),
        ),
        out_specs=P("gx", "gy", "gz", None),
        check_vma=False,
    )
```

```python
import functools

import jax
import jax.numpy as jnp
from jax import lax
from jax.experimental import pallas as pl
from jax.experimental.pallas import tpu as pltpu
from jax.sharding import PartitionSpec as P

F32 = jnp.float32
BF16 = jnp.bfloat16
STEPS = [(dx, dy) for dx in (-1, 0, 1) for dy in (-1, 0, 1)]


def span(d, n, pad):
    if d == 0:
        return pl.ds(pad, n), pl.ds(1, n)
    if d < 0:
        return pl.ds(pad, 1), pl.ds(n + 1, 1)
    return pl.ds(pad + n - 1, 1), pl.ds(0, 1)


def kernel(
    dims,
    v, wf_h, wh_h, w1_h, w2_h, wu_h,
    out,
    wf, wh, w1, w2, wu, wsem,
    p1, f1, g1, e1, t1,
    p2, f2, g2, e2,
    p3, f3, g3, e3, acc,
    pk2, l2, sel2, q2, pk3, l3, q3, pk4, l4, vup,
    s1, r1, s2, r2, s3, r3, s4, r4, s5, r5, s6, r6,
):
    gxn, gyn = dims
    gx, gy, gz = lax.axis_index("gx"), lax.axis_index("gy"), lax.axis_index("gz")
    oz = 1 - gz

    loads = [
        pltpu.make_async_copy(src, dst, wsem.at[i])
        for i, (src, dst) in enumerate(((wf_h, wf), (wh_h, wh), (w1_h, w1), (w2_h, w2), (wu_h, wu)))
    ]
    for load in loads:
        load.start()

    def on(cond, fn):
        if cond is True:
            fn()
        else:
            pl.when(cond)(fn)

    def exists(dx, dy):
        conds = []
        if dx < 0:
            conds.append(gx > 0)
        if dx > 0:
            conds.append(gx < gxn - 1)
        if dy < 0:
            conds.append(gy > 0)
        if dy > 0:
            conds.append(gy < gyn - 1)
        if not conds:
            return True
        return functools.reduce(jnp.logical_and, conds)

    for ref in (p1, g1, p2, g2, p3, g3, l2, l3, l4):
        ref[...] = jnp.zeros(ref.shape, ref.dtype)

    barrier = pltpu.get_barrier_semaphore()
    for s in range(gxn):
        there = lax.rem(gx + s, gxn)
        for dy in (-1, 0, 1):
            for z in (0, 1):
                if s == 0 and dy == 0 and z == 0:
                    continue

                def signal(there=there, dy=dy, z=z):
                    pl.semaphore_signal(
                        barrier, inc=1,
                        device_id={"gx": there, "gy": gy + dy, "gz": oz if z else gz},
                        device_id_type=pl.DeviceIdType.MESH,
                    )

                on(exists(0, dy), signal)
    lines = 1 + (gy > 0).astype(jnp.int32) + (gy < gyn - 1).astype(jnp.int32)
    pl.semaphore_wait(barrier, 2 * gxn * lines - 1)

    def send(src, dst, ss, rs, x, y, z):
        return pltpu.make_async_remote_copy(
            src_ref=src, dst_ref=dst, send_sem=ss, recv_sem=rs,
            device_id={"gx": x, "gy": y, "gz": z}, device_id_type=pl.DeviceIdType.MESH,
        )

    late = []

    def neighbours(src, pad, face, rim, side, nx, ny, ss, rs):
        arrivals = []
        for i, (dx, dy) in enumerate(STEPS):
            sx, tx = span(dx, nx, pad)
            sy, ty = span(dy, ny, pad)
            fx, _ = span(dx, nx, 0)
            fy, _ = span(dy, ny, 0)
            copies = [send(face.at[fx, fy], side.at[tx, ty], ss.at[9 + i], rs.at[9 + i], gx + dx, gy + dy, oz)]
            if (dx, dy) != (0, 0):
                copies.append(send(src.at[sx, sy], rim.at[tx, ty], ss.at[i], rs.at[i], gx + dx, gy + dy, gz))
            for copy in copies:
                on(exists(dx, dy), copy.start)
                late.append((exists(dx, dy), copy.wait_send))
                arrivals.append((exists(-dx, -dy), copy.wait_recv))

        def wait():
            for cond, fn in arrivals:
                on(cond, fn)

        return wait

    def edge(block):
        size = block.shape[-2]
        rows = lax.broadcasted_iota(jnp.int32, block.shape, block.ndim - 2)
        return jnp.sum(jnp.where(rows == (size - 1) * oz, block, 0.0), axis=block.ndim - 2, keepdims=True)

    def shifted(block, fill):
        size = block.shape[-2]
        axis = block.ndim - 2
        rows = lax.broadcasted_iota(jnp.int32, block.shape, axis)
        below = jnp.where(rows == 0, 0.0, pltpu.roll(block, 1, axis))
        above = jnp.where(rows == size - 1, 0.0, pltpu.roll(block, size - 1, axis))
        if fill is not None:
            fill = jnp.broadcast_to(fill, block.shape)
            below = jnp.where(rows == jnp.where(gz == 1, 0, -1), fill, below)
            above = jnp.where(rows == jnp.where(gz == 0, size - 1, -1), fill, above)
        return below, above

    def rounded(x):
        return x.astype(BF16).astype(F32)

    nx, ny, nz, c0 = v.shape
    for x in range(nx):
        f1[x] = edge(v[x].astype(F32))
    arrived = neighbours(v, 0, f1, p1, g1, nx, ny, s1, r1)
    p1[1 : nx + 1, 1 : ny + 1] = v[...]
    arrived()

    @pl.loop(0, nx + 2)
    def _(x):
        block = p1[x].astype(F32)
        below, above = shifted(block, g1[x])
        e1[x, :, :, 0:c0] = below.astype(BF16)
        e1[x, :, :, c0 : 2 * c0] = p1[x]
        e1[x, :, :, 2 * c0 :] = above.astype(BF16)

    loads[0].wait()

    def full_row(x):
        total = jnp.zeros((ny * nz, c0), F32)
        for ox in range(3):
            for oy in range(3):
                lhs = e1[x + ox, oy : oy + ny].reshape(ny * nz, 3 * c0)
                total = total + jnp.dot(lhs, wf[ox * 3 + oy], preferred_element_type=F32)
        return jnp.maximum(total, 0.0)

    hx, hy, hz = nx // 2, ny // 2, nz // 2

    @pl.loop(0, hx)
    def _(x):
        both = jnp.maximum(full_row(2 * x), full_row(2 * x + 1)).reshape(hy, 2, nz, c0)
        t1[...] = jnp.max(both, axis=1)
        small = jnp.maximum(t1[:, pl.ds(0, hz, stride=2), :], t1[:, pl.ds(1, hz, stride=2), :])
        small = rounded(small)
        p2[x + 1, 1 : hy + 1] = small
        f2[x] = edge(small)

    arrived = neighbours(p2, 1, f2, p2, g2, hx, hy, s2, r2)
    arrived()
    for x in range(hx + 2):
        block = p2[x]
        below, above = shifted(block, g2[x])
        e2[0, x], e2[1, x], e2[2, x] = below, block, above
    loads[1].wait()
    rows = hx * hy * hz
    c1 = wh.shape[2]
    total = jnp.zeros((rows, c1), F32)
    for ox in range(3):
        for oy in range(3):
            for k in range(3):
                lhs = e2[k, ox : ox + hx, oy : oy + hy].reshape(rows, c0).astype(BF16)
                total = total + jnp.dot(lhs, wh[(ox * 3 + oy) * 3 + k], preferred_element_type=F32)
    skip = rounded(jnp.maximum(total, 0.0)).reshape(hx, hy, hz, c1)
    p3[1 : hx + 1, 1 : hy + 1] = skip
    f3[...] = edge(skip)

    cx, cy, cz = hx // 2, hy // 2, hz // 2
    ax = gxn * cx
    group = cz * cx
    m = jnp.max(skip.reshape(cx, 2, cy, 2, hz, c1), axis=(1, 3))
    m = m.reshape(cx * cy * hz, c1)
    m = jnp.maximum(m, pltpu.roll(m, m.shape[0] - 1, 0)).astype(BF16)

    blocks = []
    lane = lax.broadcasted_iota(jnp.int32, (group, cx * cy * hz), 1)
    sub = lax.broadcasted_iota(jnp.int32, (group, cx * cy * hz), 0)
    shift_x = cx.bit_length() - 1
    sub_x = sub & (cx - 1)
    sub_o = sub >> shift_x
    for y in range(cy):
        blocks.append(jnp.where(lane == (sub_x * cy + y) * hz + 2 * sub_o, 1.0, 0.0))
    blocks.append(jnp.where(lane == (sub_x * cy + sub_o) * hz + 2 * (cz - 1) * oz, 1.0, 0.0))
    pick = jnp.concatenate(blocks, axis=0).astype(BF16)
    packets = jnp.dot(pick, m, preferred_element_type=F32).reshape(cy + 1, group, c1).astype(BF16)
    pk2[...] = packets
    l2[gx, 0:cy] = packets[0:cy]

    slots = cy + 5

    def coarse_copy(s, dy, z, k):
        def make(src_gx, tgt_gx):
            if z == 0:
                src = {0: pl.ds(0, cy), -1: pl.ds(0, 1), 1: pl.ds(cy - 1, 1)}[dy]
                dst = {0: pl.ds(0, cy), 1: pl.ds(cy, 1), -1: pl.ds(cy + 1, 1)}[dy]
            else:
                src = pl.ds(cy, 1)
                dst = {0: pl.ds(cy + 2, 1), 1: pl.ds(cy + 3, 1), -1: pl.ds(cy + 4, 1)}[dy]
            return send(pk2.at[src], l2.at[src_gx, dst], s4.at[s, k], r4.at[s, k], tgt_gx, gy + dy, oz if z else gz)

        return make

    def deep_copy(pk, land, ss, rs):
        def choose(s, dy, z, k):
            def make(src_gx, tgt_gx):
                sy, ty = span(dy, cy, 0)
                sender = gz if src_gx is gx else (oz if z else gz)
                if z == 0:
                    src = pk.at[sy]
                    dst = land.at[src_gx, ty, pl.ds(1, cz)]
                else:
                    src = pk.at[sy, pl.ds((cz - 1) * (1 - sender), 1)]
                    dst = land.at[src_gx, ty, pl.ds((cz + 1) * sender, 1)]
                return send(src, dst, ss.at[s, k], rs.at[s, k], tgt_gx, gy + dy, oz if z else gz)

            return make

        return choose

    def narrow_copy(s, dy, z, k):
        def make(src_gx, tgt_gx):
            sy, ty = span(dy, cy, 0)
            sender = gz if src_gx is gx else (oz if z else gz)
            if z == 0:
                src = pk4.at[tgt_gx, sy]
                dst = l4.at[src_gx, ty, pl.ds(1, cz // 2)]
            else:
                src = pk4.at[tgt_gx, sy, pl.ds((cz // 2 - 1) * (1 - sender), 1)]
                dst = l4.at[src_gx, ty, pl.ds((cz // 2 + 1) * sender, 1)]
            return send(src, dst, s6.at[s, k], r6.at[s, k], tgt_gx, gy + dy, oz if z else gz)

        return make

    def column_exchange(choose):
        arrivals = []
        for s in list(range(1, gxn)) + [0]:
            there = lax.rem(gx + s, gxn)
            origin = lax.rem(gx + gxn - s, gxn)
            for k, (dy, z) in enumerate(((0, 0), (-1, 0), (1, 0), (0, 1), (-1, 1), (1, 1))):
                if s == 0 and k == 0:
                    continue
                make = choose(s, dy, z, k)
                copy = make(gx, there)
                on(exists(0, dy), copy.start)
                late.append((exists(0, dy), copy.wait_send))
                arrivals.append((exists(0, -dy), make(origin, there).wait_recv))

        def wait():
            for cond, fn in arrivals:
                on(cond, fn)

        return wait

    arrived = column_exchange(coarse_copy)

    span_g = slots * group
    width = gxn * span_g
    lane = lax.broadcasted_iota(jnp.int32, (ax, width), 1)
    xs = lax.broadcasted_iota(jnp.int32, (ax, width), 0)
    base = lane - ((xs >> shift_x) * span_g + (xs & (cx - 1)))
    for y in range(-1, cy + 1):
        for z in range(-1, cz + 1):
            if 0 <= z < cz:
                slot = y if 0 <= y < cy else (cy if y < 0 else cy + 1)
                at = slot * group + z * cx
            else:
                slot = cy + 2 if 0 <= y < cy else (cy + 3 if y < 0 else cy + 4)
                line = y if 0 <= y < cy else (cy - 1 if y < 0 else 0)
                mine = (gz == 1) if z < 0 else (gz == 0)
                at = jnp.where(mine, slot * group + line * cx, -width * 4)
            sel2[y + 1, z + 1] = jnp.where(base == at, 1.0, 0.0)

    rim = (cy + 2) * (cz + 2) * ax
    select = sel2[...].reshape(rim, width).astype(BF16)
    arrived()
    skip_arrived = neighbours(p3, 1, f3, p3, g3, hx, hy, s3, r3)
    landed = l2[...].astype(F32).reshape(width, c1).astype(BF16)
    block = jnp.dot(select, landed, preferred_element_type=F32).reshape(cy + 2, cz + 2, ax, c1)

    def spread(q, block):
        below, above = shifted(block, None)
        q[0], q[1], q[2] = below, block, above

    deep = cy * cz * ax
    fo = w1.shape[2]

    def bottom(q, w):
        total = jnp.zeros((deep, fo), F32)
        for ox in range(3):
            for oy in range(3):
                for k in range(3):
                    lhs = q[ox, oy : oy + cy, k : k + cz].reshape(deep, q.shape[-1]).astype(BF16)
                    total = total + jnp.dot(lhs, w[(ox * 3 + oy) * 3 + k], preferred_element_type=F32)
        return jnp.maximum(total, 0.0).reshape(cy, cz, ax, fo).astype(BF16)

    spread(q2, block)
    loads[2].wait()
    first = bottom(q2, w1)
    pk3[...] = first
    l3[gx, 1 : cy + 1, 1 : cz + 1] = first
    arrived = column_exchange(deep_copy(pk3, l3, s5, r5))

    skip_arrived()
    for x in range(hx + 2):
        block = p3[x]
        below, above = shifted(block, g3[x])
        e3[0, x], e3[1, x], e3[2, x] = below, block, above
    loads[4].wait()
    c2 = w2.shape[1]
    total = jnp.zeros((rows, c1), F32)
    for ox in range(3):
        for oy in range(3):
            for k in range(3):
                lhs = e3[k, ox : ox + hx, oy : oy + hy].reshape(rows, c1).astype(BF16)
                total = total + jnp.dot(lhs, wu[(ox * 3 + oy) * 3 + k, c2:, :], preferred_element_type=F32)
    acc[...] = total.reshape(hx, hy, hz, c1)

    near = cx + 2
    wide = gxn * cz * near
    lane = lax.broadcasted_iota(jnp.int32, (wide, cz * ax), 1)
    row = lax.broadcasted_iota(jnp.int32, (wide, cz * ax), 0)
    shift_n = near.bit_length() - 1
    shift_z = cz.bit_length() - 1
    at = (row >> (shift_n + shift_z)) * cx + (row & (near - 1)) - 1
    at = jnp.where(jnp.logical_and(at >= 0, at < ax), at, -(cz + 1) * ax)
    share = jnp.where(lane == ((row >> shift_n) & (cz - 1)) * ax + at, 1.0, 0.0).astype(BF16)

    lane = lax.broadcasted_iota(jnp.int32, (hz, (cz + 4) * near), 1)
    zs = lax.broadcasted_iota(jnp.int32, (hz, (cz + 4) * near), 0)
    blocks = []
    for k in range(3):
        for x in range(-1, hx + 1):
            blocks.append(jnp.where(lane == (((zs + (k - 1)) >> 1) + 2) * near + (x >> 1) + 1, 1.0, 0.0))
    pick = jnp.concatenate(blocks, axis=0).astype(BF16)

    arrived()
    spread(q3, jnp.concatenate([l3[g].astype(F32) for g in range(gxn)], axis=-1))
    loads[3].wait()
    second = bottom(q3, w2)
    for y in range(cy):
        line = second[y].astype(F32).reshape(cz * ax, fo).astype(BF16)
        line = jnp.dot(share, line, preferred_element_type=F32)
        pk4[:, y] = line.reshape(gxn, cz // 2, 2 * near, fo).astype(BF16)
    l4[gx, 1 : cy + 1, 1 : cz // 2 + 1] = pk4[gx]
    arrived = column_exchange(narrow_copy)
    arrived()
    for y in range(cy + 2):
        field = jnp.concatenate([l4[g, y].astype(F32) for g in range(gxn)], axis=-1)
        field = field.reshape((cz + 4) * near, c2).astype(BF16)
        vup[:, y] = jnp.dot(pick, field, preferred_element_type=F32).reshape(3, hx + 2, hz, c2)

    parts = []
    for oy in range(3):
        low, high = (oy + 1) // 2, (hy - 1 + oy + 1) // 2 + 1
        count = high - low
        total = jnp.zeros((count * hx * hz, c1), F32)
        for ox in range(3):
            for k in range(3):
                lhs = vup[k, low:high, ox : ox + hx].reshape(count * hx * hz, c2).astype(BF16)
                total = total + jnp.dot(lhs, wu[(ox * 3 + oy) * 3 + k, :c2, :], preferred_element_type=F32)
        parts.append((low, total.reshape(count, hx, hz, c1)))
    for y in range(hy):
        line = acc[:, y]
        for oy in range(3):
            low, part = parts[oy]
            line = line + part[(y + oy + 1) // 2 - low]
        out[:, y] = line.astype(BF16)

    for cond, fn in late:
        on(cond, fn)


def on_device(dims, volume, w_full, w_half, w_bottom_in, w_bottom_out, w_up):
    gxn, gyn = dims
    nx, ny, nz, c0 = volume.shape
    c1 = w_half.shape[4]
    c2, fo = w_bottom_out.shape[3:]
    hx, hy, hz = nx // 2, ny // 2, nz // 2
    cx, cy, cz = hx // 2, hy // 2, hz // 2
    ax = gxn * cx
    weights = [
        w_full.reshape(9, 3 * c0, c0),
        w_half.reshape(27, c0, c1),
        w_bottom_in.reshape(27, c1, fo),
        w_bottom_out.reshape(27, c2, fo),
        w_up.reshape(27, c2 + c1, c1),
    ]
    vm = pltpu.VMEM
    dma = pltpu.SemaphoreType.DMA
    scratch = [vm(w.shape, BF16) for w in weights] + [dma((5,))]
    scratch += [
        vm((nx + 2, ny + 2, nz, c0), BF16), vm((nx, ny, 1, c0), F32), vm((nx + 2, ny + 2, 1, c0), F32),
        vm((nx + 2, ny + 2, nz, 3 * c0), BF16), vm((hy, nz, c0), F32),
        vm((hx + 2, hy + 2, hz, c0), F32), vm((hx, hy, 1, c0), F32), vm((hx + 2, hy + 2, 1, c0), F32),
        vm((3, hx + 2, hy + 2, hz, c0), F32),
        vm((hx + 2, hy + 2, hz, c1), F32), vm((hx, hy, 1, c1), F32), vm((hx + 2, hy + 2, 1, c1), F32),
        vm((3, hx + 2, hy + 2, hz, c1), F32), vm((hx, hy, hz, c1), F32),
        vm((cy + 1, cz * cx, c1), BF16), vm((gxn, cy + 5, cz * cx, c1), BF16),
        vm((cy + 2, cz + 2, ax, gxn * (cy + 5) * cz * cx), F32), vm((3, cy + 2, cz + 2, ax, c1), F32),
        vm((cy, cz, ax, fo), BF16), vm((gxn, cy + 2, cz + 2, ax, fo), BF16), vm((3, cy + 2, cz + 2, ax, c2), F32),
        vm((gxn, cy, cz // 2, 2 * (cx + 2), fo), BF16), vm((gxn, cy + 2, cz // 2 + 2, 2 * (cx + 2), fo), BF16),
        vm((3, cy + 2, hx + 2, hz, c2), F32),
    ]
    scratch += [dma((18,))] * 6 + [dma((gxn, 6))] * 6
    return pl.pallas_call(
        functools.partial(kernel, dims),
        out_shape=jax.ShapeDtypeStruct((hx, hy, hz, c1), BF16),
        in_specs=[pl.BlockSpec(memory_space=pltpu.VMEM)] + [pl.BlockSpec(memory_space=pl.ANY)] * 5,
        out_specs=pl.BlockSpec(memory_space=pltpu.VMEM),
        scratch_shapes=scratch,
        compiler_params=pltpu.CompilerParams(
            collective_id=0, has_side_effects=True, vmem_limit_bytes=60 * 1024 * 1024
        ),
    )(volume, *weights)


def solution(mesh):
    dims = (mesh.shape["gx"], mesh.shape["gy"])
    assert mesh.shape["gz"] == 2
    return jax.shard_map(
        functools.partial(on_device, dims),
        mesh=mesh,
        in_specs=(
            P("gx", "gy", "gz", None),
            P(),
            P(),
            P(None, None, None, None, "gx"),
            P(None, None, None, None, "gx"),
            P(),
        ),
        out_specs=P("gx", "gy", "gz", None),
        check_vma=False,
    )
```

```python
import functools

import jax
import jax.numpy as jnp
from jax import lax
from jax.experimental import pallas as pl
from jax.experimental.pallas import tpu as pltpu
from jax.sharding import PartitionSpec as P

F32 = jnp.float32
BF16 = jnp.bfloat16
STEPS = [(dx, dy) for dx in (-1, 0, 1) for dy in (-1, 0, 1)]


def span(d, n, pad):
    if d == 0:
        return pl.ds(pad, n), pl.ds(1, n)
    if d < 0:
        return pl.ds(pad, 1), pl.ds(n + 1, 1)
    return pl.ds(pad + n - 1, 1), pl.ds(0, 1)


def kernel(
    dims,
    v, wf_h, wh_h, w1_h, w2_h, wu_h,
    out,
    wf, wh, w1, w2, wu, wsem, wt,
    p1, f1, g1, e1, t1,
    p2, f2, g2, e2,
    p3, f3, g3, e3, acc,
    pk2, l2, sel2, q2, pk3, l3, q3, pk4, l4, vup,
    s1, r1, s2, r2, s3, r3, s4, r4, s5, r5, s6, r6,
):
    gxn, gyn = dims
    gx, gy, gz = lax.axis_index("gx"), lax.axis_index("gy"), lax.axis_index("gz")
    oz = 1 - gz

    loads = [
        pltpu.make_async_copy(src, dst, wsem.at[i])
        for i, (src, dst) in enumerate(((wf_h, wf), (wh_h, wh), (w1_h, w1), (w2_h, w2), (wu_h, wu)))
    ]
    for load in loads:
        load.start()

    def on(cond, fn):
        if cond is True:
            fn()
        else:
            pl.when(cond)(fn)

    def exists(dx, dy):
        conds = []
        if dx < 0:
            conds.append(gx > 0)
        if dx > 0:
            conds.append(gx < gxn - 1)
        if dy < 0:
            conds.append(gy > 0)
        if dy > 0:
            conds.append(gy < gyn - 1)
        if not conds:
            return True
        return functools.reduce(jnp.logical_and, conds)

    for ref in (p1, g1, p2, g2, p3, g3, l2, l3, l4):
        ref[...] = jnp.zeros(ref.shape, ref.dtype)

    barrier = pltpu.get_barrier_semaphore()
    for s in range(gxn):
        there = lax.rem(gx + s, gxn)
        for dy in (-1, 0, 1):
            for z in (0, 1):
                if s == 0 and dy == 0 and z == 0:
                    continue

                def signal(there=there, dy=dy, z=z):
                    pl.semaphore_signal(
                        barrier, inc=1,
                        device_id={"gx": there, "gy": gy + dy, "gz": oz if z else gz},
                        device_id_type=pl.DeviceIdType.MESH,
                    )

                on(exists(0, dy), signal)
    lines = 1 + (gy > 0).astype(jnp.int32) + (gy < gyn - 1).astype(jnp.int32)
    pl.semaphore_wait(barrier, 2 * gxn * lines - 1)

    def send(src, dst, ss, rs, x, y, z):
        return pltpu.make_async_remote_copy(
            src_ref=src, dst_ref=dst, send_sem=ss, recv_sem=rs,
            device_id={"gx": x, "gy": y, "gz": z}, device_id_type=pl.DeviceIdType.MESH,
        )

    late = []

    def neighbours(src, pad, face, rim, side, nx, ny, ss, rs):
        arrivals = []
        for i, (dx, dy) in enumerate(STEPS):
            sx, tx = span(dx, nx, pad)
            sy, ty = span(dy, ny, pad)
            fx, _ = span(dx, nx, 0)
            fy, _ = span(dy, ny, 0)
            copies = [send(face.at[fx, fy], side.at[tx, ty], ss.at[9 + i], rs.at[9 + i], gx + dx, gy + dy, oz)]
            if (dx, dy) != (0, 0):
                copies.append(send(src.at[sx, sy], rim.at[tx, ty], ss.at[i], rs.at[i], gx + dx, gy + dy, gz))
            for copy in copies:
                on(exists(dx, dy), copy.start)
                late.append((exists(dx, dy), copy.wait_send))
                arrivals.append((exists(-dx, -dy), copy.wait_recv))

        def wait():
            for cond, fn in arrivals:
                on(cond, fn)

        return wait

    def edge(block):
        size = block.shape[-2]
        rows = lax.broadcasted_iota(jnp.int32, block.shape, block.ndim - 2)
        return jnp.sum(jnp.where(rows == (size - 1) * oz, block, 0.0), axis=block.ndim - 2, keepdims=True)

    def shifted(block, fill):
        size = block.shape[-2]
        axis = block.ndim - 2
        rows = lax.broadcasted_iota(jnp.int32, block.shape, axis)
        below = jnp.where(rows == 0, 0.0, pltpu.roll(block, 1, axis))
        above = jnp.where(rows == size - 1, 0.0, pltpu.roll(block, size - 1, axis))
        if fill is not None:
            fill = jnp.broadcast_to(fill, block.shape)
            below = jnp.where(rows == jnp.where(gz == 1, 0, -1), fill, below)
            above = jnp.where(rows == jnp.where(gz == 0, size - 1, -1), fill, above)
        return below, above

    def rounded(x):
        return x.astype(BF16).astype(F32)

    nx, ny, nz, c0 = v.shape
    for x in range(nx):
        f1[x] = edge(v[x].astype(F32))
    arrived = neighbours(v, 0, f1, p1, g1, nx, ny, s1, r1)
    p1[1 : nx + 1, 1 : ny + 1] = v[...]

    loads[0].wait()
    k0 = 3 * c0
    for oy in range(3):
        for plane in range(4):
            at = pl.ds(plane * k0, k0)
            wt[oy, at, :c0] = wf[plane * 3 + oy] if plane < 3 else jnp.zeros((k0, c0), BF16)
            wt[oy, at, c0:] = wf[(plane - 1) * 3 + oy] if plane > 0 else jnp.zeros((k0, c0), BF16)
    arrived()

    @pl.loop(0, nx + 2)
    def _(x):
        block = p1[x].astype(F32)
        below, above = shifted(block, g1[x])
        e1[x, :, :, 0:c0] = below.astype(BF16)
        e1[x, :, :, c0 : 2 * c0] = p1[x]
        e1[x, :, :, 2 * c0 :] = above.astype(BF16)

    def full_rows(x):
        total = jnp.zeros((ny * nz, 2 * c0), F32)
        for oy in range(3):
            for half in range(2):
                lhs = [e1[x + 2 * half + i, oy : oy + ny].reshape(ny * nz, k0) for i in range(2)]
                rhs = wt[oy, 2 * half * k0 : 2 * (half + 1) * k0]
                total = total + jnp.dot(jnp.concatenate(lhs, axis=1), rhs, preferred_element_type=F32)
        return jnp.maximum(jnp.maximum(total[:, :c0], total[:, c0:]), 0.0)

    hx, hy, hz = nx // 2, ny // 2, nz // 2

    @pl.loop(0, hx)
    def _(x):
        both = full_rows(2 * x).reshape(hy, 2, nz, c0)
        t1[...] = jnp.max(both, axis=1)
        small = jnp.maximum(t1[:, pl.ds(0, hz, stride=2), :], t1[:, pl.ds(1, hz, stride=2), :])
        small = rounded(small)
        p2[x + 1, 1 : hy + 1] = small
        f2[x] = edge(small)

    arrived = neighbours(p2, 1, f2, p2, g2, hx, hy, s2, r2)
    arrived()
    for x in range(hx + 2):
        block = p2[x]
        below, above = shifted(block, g2[x])
        e2[0, x], e2[1, x], e2[2, x] = below, block, above
    loads[1].wait()
    rows = hx * hy * hz
    c1 = wh.shape[2]
    total = jnp.zeros((rows, c1), F32)
    for ox in range(3):
        for oy in range(3):
            for k in range(3):
                lhs = e2[k, ox : ox + hx, oy : oy + hy].reshape(rows, c0).astype(BF16)
                total = total + jnp.dot(lhs, wh[(ox * 3 + oy) * 3 + k], preferred_element_type=F32)
    skip = rounded(jnp.maximum(total, 0.0)).reshape(hx, hy, hz, c1)
    p3[1 : hx + 1, 1 : hy + 1] = skip
    f3[...] = edge(skip)

    cx, cy, cz = hx // 2, hy // 2, hz // 2
    ax = gxn * cx
    group = cz * cx
    m = jnp.max(skip.reshape(cx, 2, cy, 2, hz, c1), axis=(1, 3))
    m = m.reshape(cx * cy * hz, c1)
    m = jnp.maximum(m, pltpu.roll(m, m.shape[0] - 1, 0)).astype(BF16)

    blocks = []
    lane = lax.broadcasted_iota(jnp.int32, (group, cx * cy * hz), 1)
    sub = lax.broadcasted_iota(jnp.int32, (group, cx * cy * hz), 0)
    shift_x = cx.bit_length() - 1
    sub_x = sub & (cx - 1)
    sub_o = sub >> shift_x
    for y in range(cy):
        blocks.append(jnp.where(lane == (sub_x * cy + y) * hz + 2 * sub_o, 1.0, 0.0))
    blocks.append(jnp.where(lane == (sub_x * cy + sub_o) * hz + 2 * (cz - 1) * oz, 1.0, 0.0))
    pick = jnp.concatenate(blocks, axis=0).astype(BF16)
    packets = jnp.dot(pick, m, preferred_element_type=F32).reshape(cy + 1, group, c1).astype(BF16)
    pk2[...] = packets
    l2[gx, 0:cy] = packets[0:cy]

    slots = cy + 5

    def coarse_copy(s, dy, z, k):
        def make(src_gx, tgt_gx):
            if z == 0:
                src = {0: pl.ds(0, cy), -1: pl.ds(0, 1), 1: pl.ds(cy - 1, 1)}[dy]
                dst = {0: pl.ds(0, cy), 1: pl.ds(cy, 1), -1: pl.ds(cy + 1, 1)}[dy]
            else:
                src = pl.ds(cy, 1)
                dst = {0: pl.ds(cy + 2, 1), 1: pl.ds(cy + 3, 1), -1: pl.ds(cy + 4, 1)}[dy]
            return send(pk2.at[src], l2.at[src_gx, dst], s4.at[s, k], r4.at[s, k], tgt_gx, gy + dy, oz if z else gz)

        return make

    def deep_copy(pk, land, ss, rs):
        def choose(s, dy, z, k):
            def make(src_gx, tgt_gx):
                sy, ty = span(dy, cy, 0)
                sender = gz if src_gx is gx else (oz if z else gz)
                if z == 0:
                    src = pk.at[sy]
                    dst = land.at[src_gx, ty, pl.ds(1, cz)]
                else:
                    src = pk.at[sy, pl.ds((cz - 1) * (1 - sender), 1)]
                    dst = land.at[src_gx, ty, pl.ds((cz + 1) * sender, 1)]
                return send(src, dst, ss.at[s, k], rs.at[s, k], tgt_gx, gy + dy, oz if z else gz)

            return make

        return choose

    def narrow_copy(s, dy, z, k):
        def make(src_gx, tgt_gx):
            sy, ty = span(dy, cy, 0)
            sender = gz if src_gx is gx else (oz if z else gz)
            if z == 0:
                src = pk4.at[tgt_gx, sy]
                dst = l4.at[src_gx, ty, pl.ds(1, cz // 2)]
            else:
                src = pk4.at[tgt_gx, sy, pl.ds((cz // 2 - 1) * (1 - sender), 1)]
                dst = l4.at[src_gx, ty, pl.ds((cz // 2 + 1) * sender, 1)]
            return send(src, dst, s6.at[s, k], r6.at[s, k], tgt_gx, gy + dy, oz if z else gz)

        return make

    def column_exchange(choose):
        arrivals = []
        for s in list(range(1, gxn)) + [0]:
            there = lax.rem(gx + s, gxn)
            origin = lax.rem(gx + gxn - s, gxn)
            for k, (dy, z) in enumerate(((0, 0), (-1, 0), (1, 0), (0, 1), (-1, 1), (1, 1))):
                if s == 0 and k == 0:
                    continue
                make = choose(s, dy, z, k)
                copy = make(gx, there)
                on(exists(0, dy), copy.start)
                late.append((exists(0, dy), copy.wait_send))
                arrivals.append((exists(0, -dy), make(origin, there).wait_recv))

        def wait():
            for cond, fn in arrivals:
                on(cond, fn)

        return wait

    arrived = column_exchange(coarse_copy)

    span_g = slots * group
    width = gxn * span_g
    lane = lax.broadcasted_iota(jnp.int32, (ax, width), 1)
    xs = lax.broadcasted_iota(jnp.int32, (ax, width), 0)
    base = lane - ((xs >> shift_x) * span_g + (xs & (cx - 1)))
    for y in range(-1, cy + 1):
        for z in range(-1, cz + 1):
            if 0 <= z < cz:
                slot = y if 0 <= y < cy else (cy if y < 0 else cy + 1)
                at = slot * group + z * cx
            else:
                slot = cy + 2 if 0 <= y < cy else (cy + 3 if y < 0 else cy + 4)
                line = y if 0 <= y < cy else (cy - 1 if y < 0 else 0)
                mine = (gz == 1) if z < 0 else (gz == 0)
                at = jnp.where(mine, slot * group + line * cx, -width * 4)
            sel2[y + 1, z + 1] = jnp.where(base == at, 1.0, 0.0)

    rim = (cy + 2) * (cz + 2) * ax
    select = sel2[...].reshape(rim, width).astype(BF16)
    arrived()
    skip_arrived = neighbours(p3, 1, f3, p3, g3, hx, hy, s3, r3)
    landed = l2[...].astype(F32).reshape(width, c1).astype(BF16)
    block = jnp.dot(select, landed, preferred_element_type=F32).reshape(cy + 2, cz + 2, ax, c1)

    def spread(q, block):
        below, above = shifted(block, None)
        q[0], q[1], q[2] = below, block, above

    deep = cy * cz * ax
    fo = w1.shape[2]

    def bottom(q, w):
        total = jnp.zeros((deep, fo), F32)
        for ox in range(3):
            for oy in range(3):
                for k in range(3):
                    lhs = q[ox, oy : oy + cy, k : k + cz].reshape(deep, q.shape[-1]).astype(BF16)
                    total = total + jnp.dot(lhs, w[(ox * 3 + oy) * 3 + k], preferred_element_type=F32)
        return jnp.maximum(total, 0.0).reshape(cy, cz, ax, fo).astype(BF16)

    spread(q2, block)
    loads[2].wait()
    first = bottom(q2, w1)
    pk3[...] = first
    l3[gx, 1 : cy + 1, 1 : cz + 1] = first
    arrived = column_exchange(deep_copy(pk3, l3, s5, r5))

    skip_arrived()
    for x in range(hx + 2):
        block = p3[x]
        below, above = shifted(block, g3[x])
        e3[0, x], e3[1, x], e3[2, x] = below, block, above
    loads[4].wait()
    c2 = w2.shape[1]
    total = jnp.zeros((rows, c1), F32)
    for ox in range(3):
        for oy in range(3):
            for k in range(3):
                lhs = e3[k, ox : ox + hx, oy : oy + hy].reshape(rows, c1).astype(BF16)
                total = total + jnp.dot(lhs, wu[(ox * 3 + oy) * 3 + k, c2:, :], preferred_element_type=F32)
    acc[...] = total.reshape(hx, hy, hz, c1)

    near = cx + 2
    wide = gxn * cz * near
    lane = lax.broadcasted_iota(jnp.int32, (wide, cz * ax), 1)
    row = lax.broadcasted_iota(jnp.int32, (wide, cz * ax), 0)
    shift_n = near.bit_length() - 1
    shift_z = cz.bit_length() - 1
    at = (row >> (shift_n + shift_z)) * cx + (row & (near - 1)) - 1
    at = jnp.where(jnp.logical_and(at >= 0, at < ax), at, -(cz + 1) * ax)
    share = jnp.where(lane == ((row >> shift_n) & (cz - 1)) * ax + at, 1.0, 0.0).astype(BF16)

    lane = lax.broadcasted_iota(jnp.int32, (hz, (cz + 4) * near), 1)
    zs = lax.broadcasted_iota(jnp.int32, (hz, (cz + 4) * near), 0)
    blocks = []
    for k in range(3):
        for x in range(-1, hx + 1):
            blocks.append(jnp.where(lane == (((zs + (k - 1)) >> 1) + 2) * near + (x >> 1) + 1, 1.0, 0.0))
    pick = jnp.concatenate(blocks, axis=0).astype(BF16)

    arrived()
    spread(q3, jnp.concatenate([l3[g].astype(F32) for g in range(gxn)], axis=-1))
    loads[3].wait()
    second = bottom(q3, w2)
    for y in range(cy):
        line = second[y].astype(F32).reshape(cz * ax, fo).astype(BF16)
        line = jnp.dot(share, line, preferred_element_type=F32)
        pk4[:, y] = line.reshape(gxn, cz // 2, 2 * near, fo).astype(BF16)
    l4[gx, 1 : cy + 1, 1 : cz // 2 + 1] = pk4[gx]
    arrived = column_exchange(narrow_copy)
    arrived()
    for y in range(cy + 2):
        field = jnp.concatenate([l4[g, y].astype(F32) for g in range(gxn)], axis=-1)
        field = field.reshape((cz + 4) * near, c2).astype(BF16)
        vup[:, y] = jnp.dot(pick, field, preferred_element_type=F32).reshape(3, hx + 2, hz, c2)

    parts = []
    for oy in range(3):
        low, high = (oy + 1) // 2, (hy - 1 + oy + 1) // 2 + 1
        count = high - low
        total = jnp.zeros((count * hx * hz, c1), F32)
        for ox in range(3):
            for k in range(3):
                lhs = vup[k, low:high, ox : ox + hx].reshape(count * hx * hz, c2).astype(BF16)
                total = total + jnp.dot(lhs, wu[(ox * 3 + oy) * 3 + k, :c2, :], preferred_element_type=F32)
        parts.append((low, total.reshape(count, hx, hz, c1)))
    for y in range(hy):
        line = acc[:, y]
        for oy in range(3):
            low, part = parts[oy]
            line = line + part[(y + oy + 1) // 2 - low]
        out[:, y] = line.astype(BF16)

    for cond, fn in late:
        on(cond, fn)


def on_device(dims, volume, w_full, w_half, w_bottom_in, w_bottom_out, w_up):
    gxn, gyn = dims
    nx, ny, nz, c0 = volume.shape
    c1 = w_half.shape[4]
    c2, fo = w_bottom_out.shape[3:]
    hx, hy, hz = nx // 2, ny // 2, nz // 2
    cx, cy, cz = hx // 2, hy // 2, hz // 2
    ax = gxn * cx
    weights = [
        w_full.reshape(9, 3 * c0, c0),
        w_half.reshape(27, c0, c1),
        w_bottom_in.reshape(27, c1, fo),
        w_bottom_out.reshape(27, c2, fo),
        w_up.reshape(27, c2 + c1, c1),
    ]
    vm = pltpu.VMEM
    dma = pltpu.SemaphoreType.DMA
    scratch = [vm(w.shape, BF16) for w in weights] + [dma((5,)), vm((3, 12 * c0, 2 * c0), BF16)]
    scratch += [
        vm((nx + 2, ny + 2, nz, c0), BF16), vm((nx, ny, 1, c0), F32), vm((nx + 2, ny + 2, 1, c0), F32),
        vm((nx + 2, ny + 2, nz, 3 * c0), BF16), vm((hy, nz, c0), F32),
        vm((hx + 2, hy + 2, hz, c0), F32), vm((hx, hy, 1, c0), F32), vm((hx + 2, hy + 2, 1, c0), F32),
        vm((3, hx + 2, hy + 2, hz, c0), F32),
        vm((hx + 2, hy + 2, hz, c1), F32), vm((hx, hy, 1, c1), F32), vm((hx + 2, hy + 2, 1, c1), F32),
        vm((3, hx + 2, hy + 2, hz, c1), F32), vm((hx, hy, hz, c1), F32),
        vm((cy + 1, cz * cx, c1), BF16), vm((gxn, cy + 5, cz * cx, c1), BF16),
        vm((cy + 2, cz + 2, ax, gxn * (cy + 5) * cz * cx), F32), vm((3, cy + 2, cz + 2, ax, c1), F32),
        vm((cy, cz, ax, fo), BF16), vm((gxn, cy + 2, cz + 2, ax, fo), BF16), vm((3, cy + 2, cz + 2, ax, c2), F32),
        vm((gxn, cy, cz // 2, 2 * (cx + 2), fo), BF16), vm((gxn, cy + 2, cz // 2 + 2, 2 * (cx + 2), fo), BF16),
        vm((3, cy + 2, hx + 2, hz, c2), F32),
    ]
    scratch += [dma((18,))] * 6 + [dma((gxn, 6))] * 6
    return pl.pallas_call(
        functools.partial(kernel, dims),
        out_shape=jax.ShapeDtypeStruct((hx, hy, hz, c1), BF16),
        in_specs=[pl.BlockSpec(memory_space=pltpu.VMEM)] + [pl.BlockSpec(memory_space=pl.ANY)] * 5,
        out_specs=pl.BlockSpec(memory_space=pltpu.VMEM),
        scratch_shapes=scratch,
        compiler_params=pltpu.CompilerParams(
            collective_id=0, has_side_effects=True, vmem_limit_bytes=60 * 1024 * 1024
        ),
    )(volume, *weights)


def solution(mesh):
    dims = (mesh.shape["gx"], mesh.shape["gy"])
    assert mesh.shape["gz"] == 2
    return jax.shard_map(
        functools.partial(on_device, dims),
        mesh=mesh,
        in_specs=(
            P("gx", "gy", "gz", None),
            P(),
            P(),
            P(None, None, None, None, "gx"),
            P(None, None, None, None, "gx"),
            P(),
        ),
        out_specs=P("gx", "gy", "gz", None),
        check_vma=False,
    )
```
